32 devices in a mesh: seq: 8 (over z, x), chan: 4 (over y, core).
Axes of the slice: x: 2, y: 2, z: 4, core: 2. Of those that a mesh axis runs over, the one named last changes fastest.
Arguments:
- hidden: bfloat16 [8, 8192], replicated, may hold values from -6 to 6
- norm_gain: float32 [3, 8192], replicated, may hold values from 0.25 to 1.75
- in_weight: bfloat16 [2, 8192, 2, 16384], P(None, None, None, ('seq', 'chan')), may hold values from -0.125 to 0.125
- conv_weight: float32 [2, 4, 16384], P(None, None, ('seq', 'chan')), may hold values from -3 to 3
- conv_bias: float32 [2, 16384], P(None, ('seq', 'chan')), may hold values from -3 to 3
- conv_state: bfloat16 [2, 8, 3, 16384], P(None, None, None, ('seq', 'chan')), may hold values from -6 to 6
- xproj_weight: bfloat16 [2, 16384, 544], P(None, ('seq', 'chan')), may hold values from -0.09375 to 0.09375
- dt_weight: bfloat16 [2, 512, 16384], P(None, None, ('seq', 'chan')), may hold values from -0.25 to 0.25
- dt_bias: float32 [2, 16384], P(None, ('seq', 'chan')), may hold values from -4.6 to -2.3
- a_log: float32 [2, 16, 16384], P(None, None, ('seq', 'chan')), may hold values from 0 to 2.77
- skip_gain: float32 [2, 16384], P(None, ('seq', 'chan')), may hold values from 0.5 to 1.5
- ssm_state: float32 [2, 8, 16, 16384], P(None, None, None, ('seq', 'chan')), may hold values from -6 to 6
- out_weight: bfloat16 [2, 16384, 8192], P(None, ('seq', 'chan')), may hold values from -0.09375 to 0.09375
- asker_lookup_matrix: bfloat16 [8192, 8, 1280], P('seq', 'chan'), may hold values from -0.0625 to 0.0625
- o_weight: bfloat16 [8, 1024, 8192], P('chan', None, 'seq'), may hold values from -0.09375 to 0.09375
- kv_cache: bfloat16 [64, 256, 2, 8, 128], P('seq', None, None, 'chan'), may hold values from -64 to 64
- lengths: int32 [8], replicated, may hold values from 1 to 2048, as said below
- page_table: int32 [8, 8], replicated, may hold values from -1 to 63, as said below
Outputs:
- hidden_out: bfloat16 [8, 8192], P(None, ('seq', 'chan'))
- new_ssm: float32 [2, 8, 16, 16384], P(None, None, None, ('seq', 'chan'))
- new_conv: bfloat16 [2, 8, 3, 16384], P(None, None, None, ('seq', 'chan'))
- newest_pair: bfloat16 [8, 8, 2, 128], P(None, 'chan')
The draws below stay inside these ranges and needn't reach their ends.
Inputs may be any that keep to these rules, and one draw needn't show every extreme that they name: `lengths`: each request's context holds 1 to 2048 tokens; one request holds exactly 2048. page_table[b, j] for j < ceil(lengths[b] / 256) is the cache slot (index along seq times 8 plus the local slot) holding block j of request b; these slots are all different; every other entry is -1. Used slots are spread very unevenly: some devices along seq have all 8 of theirs used, others few or none.
All inputs are finite; a program needn't handle non-finite values.
Results may differ from the reference program's by a relative error of at most 0.018.
Values may be sent and summed in bfloat16 or wider, within the bound.
A program may use at most 192 MiB of HBM per device.

```python
import jax
import jax.numpy as jnp
from jax import lax

D = 8192
E = 16384
N = 16
R = 512
KCONV = 4
HEADS = 64
KVH = 8
HD = 128
GROUP = 8
MAMBA_LAYERS = 2
REQ = 8
BLK = 256
PAGES_DEV = 8
SLOTS = 64
MAXPG = 8


def plan_pages(key):
    base_key = jax.random.fold_in(key, 11)
    pick_key, grow_key, ending_lock, jitter_key, rank_key = jax.random.split(base_key, 5)
    request_ids = jnp.arange(REQ, dtype=jnp.int32)
    longest = jax.random.randint(pick_key, (), 0, REQ, dtype=jnp.int32)
    short_most = (SLOTS // 2 - MAXPG) // REQ
    short_draw = jax.random.randint(grow_key, (REQ,), 0, short_most, dtype=jnp.int32)
    page_count = 1 + short_draw * short_draw // short_most
    page_count = jnp.where(request_ids == longest, MAXPG, page_count)
    tail_rows = jax.random.randint(ending_lock, (REQ,), 1, BLK + 1, dtype=jnp.int32)
    tail_rows = jnp.where(request_ids == longest, BLK, tail_rows)
    context = (page_count - 1) * BLK + tail_rows
    slot_ids = jnp.arange(SLOTS, dtype=jnp.int32)
    device_rank = jax.random.randint(rank_key, (SLOTS // PAGES_DEV,), 0, 8, dtype=jnp.int32)[slot_ids // PAGES_DEV]
    jitter = jax.random.randint(jitter_key, (SLOTS,), 0, 4096, dtype=jnp.int32)
    slot_score = (device_rank * 4096 + jitter) * SLOTS + slot_ids
    slot_order = jnp.argsort(slot_score).astype(jnp.int32)
    first_page = jnp.cumsum(page_count) - page_count
    column = jnp.arange(MAXPG, dtype=jnp.int32)
    flat_index = jnp.clip(first_page[:, None] + column[None, :], 0, SLOTS - 1)
    slot_table = jnp.where(column[None, :] < page_count[:, None], slot_order[flat_index], -1)
    return (context.astype(jnp.int32), slot_table.astype(jnp.int32))


def draw_lengths(key, part):
    return plan_pages(key)[0]


def draw_page_table(key, part):
    return plan_pages(key)[1]


def draw_kv_cache(key, part):
    cache_shape = (SLOTS, BLK, 2, KVH, HD)
    values = jnp.clip(jax.random.normal(key, cache_shape, jnp.float32), -6.0, 6.0)
    return values.astype(jnp.bfloat16)


def with_spikes(values, key, source, target, blocks, factor):
    owner, partner = [(jnp.arange(values.shape[dim]) // (values.shape[dim] // blocks)).reshape([-1 if axis == dim else 1 for axis in range(values.ndim)]) for dim in (source, target)]
    chosen = jax.random.permutation(key, blocks)[partner]
    strong = (owner == chosen) | (owner == (partner + blocks // 2) % blocks)
    return jnp.where(strong, factor * values, values)


def steps_of(key, dims, cuts, low, largest):
    level = 1.0
    for axis_at, parts in cuts:
        draws = jax.random.uniform(jax.random.fold_in(jax.random.fold_in(key, 6), axis_at), (parts,), jnp.float32, low / len(cuts), largest / len(cuts))
        level = level * jnp.repeat(jnp.exp(draws), dims[axis_at] // parts).reshape((-1,) + (1,) * (len(dims) - 1 - axis_at))
    return level


def bell_draw(rng, shape, deviation, limit, shards=(), kind=jnp.bfloat16):
    entries = deviation * jax.random.normal(rng, shape, jnp.float32)
    if shards:
        entries = entries * steps_of(rng, shape, shards, -0.22, 0.18)
    return jnp.clip(entries, -limit, limit).astype(kind)


def heavy_noise(key, shape, spread, most, cuts, heavy, kind=jnp.bfloat16):
    result = spread * jax.random.normal(key, shape, jnp.float32)
    if cuts:
        result = result * steps_of(key, shape, cuts, -0.22, 0.18)
    return jnp.clip(with_spikes(result, jax.random.fold_in(key, 3), *heavy), -most, most).astype(kind)


def setup_inputs(seed: int = 0) -> dict:
    key_of = jax.random.split(jax.random.key(seed), 19)
    hidden = bell_draw(key_of[0], (REQ, D), 1.0, 6.0)
    norm_gain = jnp.clip(1.0 + 0.15 * jax.random.normal(key_of[1], (3, D), jnp.float32), 0.25, 1.75)
    in_weight = heavy_noise(key_of[2], (MAMBA_LAYERS, D, 2, E), D ** -0.5, 0.125, ((3, 32),), (1, 3, 32, 2.75))
    conv_weight = bell_draw(key_of[3], (MAMBA_LAYERS, KCONV, E), KCONV ** -0.5, 3.0, ((2, 32),), jnp.float32)
    conv_bias = bell_draw(key_of[4], (MAMBA_LAYERS, E), 0.5, 3.0, ((1, 32),), jnp.float32)
    conv_state = bell_draw(key_of[5], (MAMBA_LAYERS, REQ, KCONV - 1, E), 1.0, 6.0, ((3, 32),))
    xproj_weight = heavy_noise(key_of[6], (MAMBA_LAYERS, E, R + 2 * N), E ** -0.5, 0.09375, ((1, 32),), (1, 2, 32, 2.75))
    dt_weight = bell_draw(key_of[7], (MAMBA_LAYERS, R, E), R ** -0.5, 0.25, ((2, 32),))
    dt_bias = jnp.clip(-4.6 + 2.3 * jax.random.uniform(key_of[8], (MAMBA_LAYERS, E), jnp.float32) ** steps_of(key_of[8], (MAMBA_LAYERS, E), ((1, 32),), -0.2, 0.2), -4.6, -2.3)
    a_log = jnp.clip(2.77 * jax.random.uniform(key_of[9], (MAMBA_LAYERS, N, E), jnp.float32) ** steps_of(key_of[9], (MAMBA_LAYERS, N, E), ((2, 32),), -0.2, 0.2), 0.0, 2.77)
    skip_gain = jnp.clip(0.5 + 1.0 * jax.random.uniform(key_of[10], (MAMBA_LAYERS, E), jnp.float32) ** steps_of(key_of[10], (MAMBA_LAYERS, E), ((1, 32),), -0.2, 0.2), 0.5, 1.5)
    ssm_state = bell_draw(key_of[11], (MAMBA_LAYERS, REQ, N, E), 1.0, 6.0, ((3, 32),), jnp.float32)
    out_weight = heavy_noise(key_of[12], (MAMBA_LAYERS, E, D), E ** -0.5, 0.09375, ((1, 32),), (1, 2, 32, 2.75))
    asker_lookup_matrix = bell_draw(key_of[13], (D, KVH, (GROUP + 2) * HD), D ** -0.5, 0.0625, ((0, 8), (1, 4)))
    o_weight = heavy_noise(key_of[14], (KVH, GROUP * HD, D), (HEADS * HD) ** -0.5, 0.09375, ((0, 4), (2, 8)), (0, 2, 8, 2.0))
    kv_cache = draw_kv_cache(jax.random.fold_in(key_of[18], 71), 0)
    lengths = draw_lengths(jax.random.fold_in(key_of[18], 71), 0)
    page_table = draw_page_table(jax.random.fold_in(key_of[18], 71), 0)
    return {"hidden": hidden, "norm_gain": norm_gain, "in_weight": in_weight, "conv_weight": conv_weight, "conv_bias": conv_bias, "conv_state": conv_state, "xproj_weight": xproj_weight, "dt_weight": dt_weight, "dt_bias": dt_bias, "a_log": a_log, "skip_gain": skip_gain, "ssm_state": ssm_state, "out_weight": out_weight, "asker_lookup_matrix": asker_lookup_matrix, "o_weight": o_weight, "kv_cache": kv_cache, "lengths": lengths, "page_table": page_table}


norm_eps = 1e-06
lowest_score = -1e+30

def normalize(stream, gain_row):
    widened = stream.astype(jnp.float32)
    inv_rms = lax.rsqrt(lax.optimization_barrier(jnp.mean(widened * widened, axis=1)) + norm_eps)
    return (widened * inv_rms[:, None] * gain_row[None, :]).astype(jnp.bfloat16)

def mamba_layer(stream, gain_row, layer, in_weight, conv_weight, conv_bias, conv_state, xproj_weight, dt_weight, dt_bias, a_log, skip_gain, ssm_state, out_weight):
    normed = normalize(stream, gain_row)
    channels = in_weight.shape[3]
    both_proj = jnp.dot(normed, in_weight[layer].reshape(in_weight.shape[1], 2 * channels), preferred_element_type=jnp.float32).astype(jnp.bfloat16)
    inputs = both_proj[:, :channels]
    gate_half = both_proj[:, channels:]
    window = jnp.concatenate([conv_state[layer], inputs[:, None, :]], axis=1)
    conv_sum = lax.optimization_barrier(jnp.sum(window.astype(jnp.float32) * conv_weight[layer][None], axis=1)) + conv_bias[layer][None, :]
    signal = lax.optimization_barrier(jax.nn.silu(conv_sum).astype(jnp.bfloat16))
    mapped_vectors = jnp.dot(signal, xproj_weight[layer], preferred_element_type=jnp.float32)
    low_rank = dt_weight.shape[1]
    state_size = a_log.shape[1]
    dt_low = mapped_vectors[:, :low_rank].astype(jnp.bfloat16)
    b_in = mapped_vectors[:, low_rank:low_rank + state_size]
    c_out = mapped_vectors[:, low_rank + state_size:]
    dt_step = jax.nn.softplus(jnp.dot(dt_low, dt_weight[layer], preferred_element_type=jnp.float32) + dt_bias[layer][None, :])
    widened = signal.astype(jnp.float32)
    decay_rate = jnp.exp(-dt_step[:, None, :] * jnp.exp(a_log[layer])[None])
    fresh_state = decay_rate * ssm_state[layer] + (dt_step * widened)[:, None, :] * b_in[:, :, None]
    readout = lax.optimization_barrier(jnp.sum(fresh_state * c_out[:, :, None], axis=1)) + skip_gain[layer][None, :] * widened
    gated_out = (readout * jax.nn.silu(gate_half.astype(jnp.float32))).astype(jnp.bfloat16)
    mixed_out = jnp.dot(gated_out, out_weight[layer], preferred_element_type=jnp.float32)
    return ((stream.astype(jnp.float32) + mixed_out).astype(jnp.bfloat16), fresh_state, window[:, 1:, :])

def attention_layer(stream, gain_row, asker_lookup_matrix, o_weight, kv_cache, lengths, page_table):
    normed = normalize(stream, gain_row)
    requests = stream.shape[0]
    heads_kv = asker_lookup_matrix.shape[1]
    per_lens_width = kv_cache.shape[4]
    group_size = asker_lookup_matrix.shape[2] // per_lens_width - 2
    inv_sqrt = per_lens_width ** (-0.5)
    qkv_all = jnp.dot(normed, asker_lookup_matrix.reshape(asker_lookup_matrix.shape[0], -1), preferred_element_type=jnp.float32)
    qkv_all = lax.optimization_barrier(qkv_all.astype(jnp.bfloat16)).reshape(requests, heads_kv, -1)
    every_question = qkv_all[:, :, :group_size * per_lens_width].reshape(requests, heads_kv, group_size, per_lens_width)
    newest_pair = qkv_all[:, :, group_size * per_lens_width:].reshape(requests, heads_kv, 2, per_lens_width)
    highest = lax.Precision.HIGHEST

    def attend_one(items):
        query_one, fresh_one, length_one, table_one = items
        page_rows = kv_cache[jnp.maximum(table_one, 0)]
        block_len = page_rows.shape[1]
        position = jnp.arange(table_one.shape[0], dtype=jnp.int32)[:, None] * block_len + jnp.arange(block_len, dtype=jnp.int32)[None, :]
        visible = (position < length_one)[None, None]
        scores = jnp.einsum('kgd,ptkd->kgpt', query_one.astype(jnp.float32), page_rows[:, :, 0].astype(jnp.float32), precision=highest) * inv_sqrt
        scores = jnp.where(visible, scores, lowest_score)
        block_top = lax.optimization_barrier(jnp.max(scores, axis=3))
        weight = jnp.where(visible, jnp.exp(scores - block_top[..., None]), 0.0)
        block_sum = lax.optimization_barrier(jnp.sum(weight, axis=3))
        rounded = lax.optimization_barrier(weight.astype(jnp.bfloat16)).astype(jnp.float32)
        block_val = jnp.einsum('kgpt,ptkd->kgpd', rounded, page_rows[:, :, 1].astype(jnp.float32), precision=highest)
        fresh_score = jnp.einsum('kgd,kd->kg', query_one.astype(jnp.float32), fresh_one[:, 0].astype(jnp.float32), precision=highest) * inv_sqrt
        final_top = jnp.maximum(lax.optimization_barrier(jnp.max(block_top, axis=2)), fresh_score)
        factor = jnp.exp(block_top - final_top[..., None])
        fresh_weight = jnp.exp(fresh_score - final_top)
        denominator = lax.optimization_barrier(jnp.sum(factor * block_sum, axis=2)) + fresh_weight
        numerator = jnp.einsum('kgp,kgpd->kgd', factor, block_val, precision=highest) + fresh_weight[..., None] * fresh_one[:, 1][:, None, :].astype(jnp.float32)
        return (numerator / denominator[..., None]).astype(jnp.bfloat16)
    attended = lax.map(attend_one, (every_question, newest_pair, lengths, page_table))
    mapped_vectors = jnp.dot(attended.reshape(requests, -1), o_weight.reshape(-1, o_weight.shape[2]), preferred_element_type=jnp.float32)
    return ((stream.astype(jnp.float32) + mapped_vectors).astype(jnp.bfloat16), newest_pair)

def reference(hidden, norm_gain, in_weight, conv_weight, conv_bias, conv_state, xproj_weight, dt_weight, dt_bias, a_log, skip_gain, ssm_state, out_weight, asker_lookup_matrix, o_weight, kv_cache, lengths, page_table):
    stream_one, state_first, conv_first = mamba_layer(hidden, norm_gain[0], 0, in_weight, conv_weight, conv_bias, conv_state, xproj_weight, dt_weight, dt_bias, a_log, skip_gain, ssm_state, out_weight)
    stream_two, newest_pair = attention_layer(stream_one, norm_gain[1], asker_lookup_matrix, o_weight, kv_cache, lengths, page_table)
    hidden_out, state_two, conv_two = mamba_layer(stream_two, norm_gain[2], 1, in_weight, conv_weight, conv_bias, conv_state, xproj_weight, dt_weight, dt_bias, a_log, skip_gain, ssm_state, out_weight)
    return (hidden_out, jnp.stack([state_first, state_two]), jnp.stack([conv_first, conv_two]), newest_pair)
```

```python
import functools

import jax
import jax.numpy as jnp
from jax import lax
from jax.experimental import pallas as pl
from jax.experimental.pallas import tpu as pltpu
from jax.sharding import PartitionSpec as P

norm_eps = 1e-06
lowest_score = -1e30
wire = jnp.bfloat16


def greet(sizes):
    barrier = pltpu.get_barrier_semaphore()
    count = 0
    for axis, size in sizes:
        me = lax.axis_index(axis)
        for hop in range(1, size):
            pl.semaphore_signal(
                barrier,
                inc=1,
                device_id={axis: lax.rem(me + hop, size)},
                device_id_type=pl.DeviceIdType.MESH,
            )
            count += 1
    pl.semaphore_wait(barrier, count)


def send_all(axis, size, source, target, send_sems, recv_sems):
    me = lax.axis_index(axis)
    copies = []
    for hop in range(1, size):
        peer = lax.rem(me + hop, size)
        copy = pltpu.make_async_remote_copy(
            src_ref=source(peer),
            dst_ref=target(hop),
            send_sem=send_sems.at[hop],
            recv_sem=recv_sems.at[hop],
            device_id={axis: peer},
            device_id_type=pl.DeviceIdType.MESH,
        )
        copy.start()
        copies.append(copy)
    return copies


def wait_all(copies):
    for copy in copies:
        copy.wait()


def summed(own, landed, size):
    total = own.astype(jnp.float32)
    for hop in range(1, size):
        total = total + landed[hop].astype(jnp.float32)
    return total


def sems(size):
    return [pltpu.SemaphoreType.DMA((size,)), pltpu.SemaphoreType.DMA((size,))]


def comm_call(kernel, outs, scratch, collective_id, *operands):
    vmem = pl.BlockSpec(memory_space=pltpu.VMEM)
    return pl.pallas_call(
        kernel,
        out_shape=outs,
        in_specs=[vmem] * len(operands),
        out_specs=jax.tree.map(lambda _: vmem, outs),
        scratch_shapes=scratch,
        compiler_params=pltpu.CompilerParams(
            collective_id=collective_id, has_side_effects=True, vmem_limit_bytes=4 * 1024 * 1024
        ),
        cost_estimate=pl.CostEstimate(flops=0, bytes_accessed=16 * 1024 * 1024, transcendentals=0),
    )(*operands)


def all_sum_kernel(sizes, x_ref, out_ref, land_a, mid, land_b, sa, ra, sb, rb):
    seq, chan = sizes
    greet((("seq", seq), ("chan", chan)))
    wait_all(send_all("chan", chan, lambda p: x_ref, lambda h: land_a.at[h], sa, ra))
    mid[...] = summed(x_ref[...], land_a, chan).astype(mid.dtype)
    wait_all(send_all("seq", seq, lambda p: mid, lambda h: land_b.at[h], sb, rb))
    out_ref[...] = summed(mid[...], land_b, seq)


def all_sum(x, collective_id):
    seq, chan = lax.axis_size("seq"), lax.axis_size("chan")
    x = x.astype(wire)
    scratch = [
        pltpu.VMEM((chan,) + x.shape, wire),
        pltpu.VMEM(x.shape, wire),
        pltpu.VMEM((seq,) + x.shape, wire),
    ]
    return comm_call(
        functools.partial(all_sum_kernel, (seq, chan)),
        jax.ShapeDtypeStruct(x.shape, jnp.float32),
        scratch + sems(chan) + sems(seq),
        collective_id,
        x,
    )


def share_sum_kernel(sizes, spread, x_ref, base_ref, out_ref, *rest):
    seq, chan = sizes
    if spread:
        block_ref, land_a, mid, land_b, sa, ra, sb, rb, sc, rc = rest
    else:
        land_a, mid, land_b, sa, ra, sb, rb = rest
    me_seq, me_chan = lax.axis_index("seq"), lax.axis_index("chan")
    greet((("seq", seq), ("chan", chan)))
    wait_all(send_all("chan", chan, lambda p: x_ref.at[p], lambda h: land_a.at[h], sa, ra))
    mid[...] = summed(x_ref[me_chan], land_a, chan).astype(mid.dtype)
    wait_all(send_all("seq", seq, lambda p: mid.at[p], lambda h: land_b.at[h], sb, rb))
    added = summed(mid[me_seq], land_b, seq)
    result = (base_ref[...].astype(jnp.float32) + added).astype(out_ref.dtype)
    out_ref[...] = result
    if spread:
        block_ref[me_chan] = result
        wait_all(
            send_all("chan", chan, lambda p: out_ref, lambda h: block_ref.at[me_chan], sc, rc)
        )


def share_sum(partial, base, spread, collective_id):
    seq, chan = lax.axis_size("seq"), lax.axis_size("chan")
    rows, width = base.shape
    x = partial.astype(wire).reshape(rows, seq, chan, width).transpose(2, 1, 0, 3)
    outs = [jax.ShapeDtypeStruct(base.shape, jnp.bfloat16)]
    scratch = [
        pltpu.VMEM((chan, seq, rows, width), wire),
        pltpu.VMEM((seq, rows, width), wire),
        pltpu.VMEM((seq, rows, width), wire),
    ]
    scratch = scratch + sems(chan) + sems(seq)
    if spread:
        outs.append(jax.ShapeDtypeStruct((chan, rows, width), jnp.bfloat16))
        scratch = scratch + sems(chan)
    return comm_call(
        functools.partial(share_sum_kernel, (seq, chan), spread),
        outs,
        scratch,
        collective_id,
        x,
        base,
    )


def seq_sum_kernel(seq, x_ref, square_ref, out_ref, squares_ref, land, mid, sa, ra, sb, rb, sc, rc):
    me = lax.axis_index("seq")
    greet((("seq", seq),))
    first = send_all("seq", seq, lambda p: x_ref.at[p], lambda h: land.at[h], sa, ra)
    second = send_all("seq", seq, lambda p: square_ref, lambda h: squares_ref.at[h], sb, rb)
    squares_ref[0] = square_ref[...]
    wait_all(first)
    total = summed(x_ref[me], land, seq).astype(mid.dtype)
    mid[...] = total
    out_ref[me] = total
    third = send_all("seq", seq, lambda p: mid, lambda h: out_ref.at[me], sc, rc)
    wait_all(second)
    wait_all(third)


def seq_sum(x, squares, collective_id):
    seq = lax.axis_size("seq")
    lanes = 128
    flat = x.astype(wire).reshape(-1, lanes)
    piece = -(-flat.shape[0] // seq)
    padded = jnp.pad(flat, ((0, piece * seq - flat.shape[0]), (0, 0))).reshape(seq, piece, lanes)
    spread = jnp.broadcast_to(squares[:, None], (squares.shape[0], lanes))
    result, gathered = comm_call(
        functools.partial(seq_sum_kernel, seq),
        [
            jax.ShapeDtypeStruct(padded.shape, wire),
            jax.ShapeDtypeStruct((seq,) + spread.shape, jnp.float32),
        ],
        [pltpu.VMEM(padded.shape, wire), pltpu.VMEM(padded.shape[1:], wire)]
        + sems(seq)
        + sems(seq)
        + sems(seq),
        collective_id,
        padded,
        spread,
    )
    whole = result.reshape(-1, lanes)[: flat.shape[0]].reshape(x.shape)
    return whole.astype(jnp.float32), jnp.sum(gathered[:, :, 0], axis=0)


def seq_collect_kernel(seq, a_ref, b_ref, a_all, b_all, sa, ra, sb, rb):
    greet((("seq", seq),))
    first = send_all("seq", seq, lambda p: b_ref, lambda h: b_all.at[h], sb, rb)
    second = send_all("seq", seq, lambda p: a_ref, lambda h: a_all.at[h], sa, ra)
    a_all[0] = a_ref[...]
    b_all[0] = b_ref[...]
    wait_all(first)
    wait_all(second)


def seq_collect(a, b, collective_id):
    seq = lax.axis_size("seq")
    return comm_call(
        functools.partial(seq_collect_kernel, seq),
        [
            jax.ShapeDtypeStruct((seq,) + a.shape, a.dtype),
            jax.ShapeDtypeStruct((seq,) + b.shape, b.dtype),
        ],
        sems(seq) + sems(seq),
        collective_id,
        a,
        b,
    )


def chan_sum_kernel(sizes, x_ref, base_ref, out_ref, all_ref, land, sa, ra, sb, rb, sc, rc):
    seq, chan = sizes
    me_seq, me_chan = lax.axis_index("seq"), lax.axis_index("chan")
    greet((("seq", seq), ("chan", chan)))
    wait_all(send_all("chan", chan, lambda p: x_ref.at[p], lambda h: land.at[h], sa, ra))
    added = summed(x_ref[me_chan], land, chan)
    result = (base_ref[...].astype(jnp.float32) + added).astype(out_ref.dtype)
    out_ref[...] = result
    all_ref[me_seq, me_chan] = result
    wait_all(
        send_all("chan", chan, lambda p: out_ref, lambda h: all_ref.at[me_seq, me_chan], sb, rb)
    )
    mine = all_ref.at[me_seq]
    wait_all(send_all("seq", seq, lambda p: mine, lambda h: all_ref.at[me_seq], sc, rc))


def chan_sum(partial, base, collective_id):
    seq, chan = lax.axis_size("seq"), lax.axis_size("chan")
    rows, width = base.shape
    x = partial.astype(wire).reshape(rows, chan, width).transpose(1, 0, 2)
    share, every = comm_call(
        functools.partial(chan_sum_kernel, (seq, chan)),
        [
            jax.ShapeDtypeStruct(base.shape, jnp.bfloat16),
            jax.ShapeDtypeStruct((seq, chan, rows, width), jnp.bfloat16),
        ],
        [pltpu.VMEM(x.shape, wire)] + sems(chan) + sems(chan) + sems(seq),
        collective_id,
        x,
        base,
    )
    return share, every.transpose(2, 0, 1, 3).reshape(rows, seq * chan * width)


def normalize(stream, gain_row):
    widened = stream.astype(jnp.float32)
    inv_rms = lax.rsqrt(jnp.mean(widened * widened, axis=1) + norm_eps)
    return (widened * inv_rms[:, None] * gain_row[None, :]).astype(jnp.bfloat16)


def mamba_mix(normed, layer, params):
    (
        in_weight,
        conv_weight,
        conv_bias,
        conv_state,
        xproj_weight,
        dt_weight,
        dt_bias,
        a_log,
        skip_gain,
        ssm_state,
    ) = params
    channels = in_weight.shape[3]
    both_proj = jnp.dot(
        normed,
        in_weight[layer].reshape(in_weight.shape[1], 2 * channels),
        preferred_element_type=jnp.float32,
    ).astype(jnp.bfloat16)
    inputs = both_proj[:, :channels]
    gate_half = both_proj[:, channels:]
    window = jnp.concatenate([conv_state[layer], inputs[:, None, :]], axis=1)
    conv_sum = (
        jnp.sum(window.astype(jnp.float32) * conv_weight[layer][None], axis=1)
        + conv_bias[layer][None, :]
    )
    signal = lax.optimization_barrier(jax.nn.silu(conv_sum).astype(jnp.bfloat16))
    x_terms = jnp.dot(signal, xproj_weight[layer], preferred_element_type=jnp.float32)
    mapped_vectors = all_sum(x_terms, 10 + layer)
    low_rank = dt_weight.shape[1]
    state_size = a_log.shape[1]
    dt_low = mapped_vectors[:, :low_rank].astype(jnp.bfloat16)
    b_in = mapped_vectors[:, low_rank : low_rank + state_size]
    c_out = mapped_vectors[:, low_rank + state_size :]
    dt_step = jax.nn.softplus(
        jnp.dot(dt_low, dt_weight[layer], preferred_element_type=jnp.float32)
        + dt_bias[layer][None, :]
    )
    widened = signal.astype(jnp.float32)
    decay_rate = jnp.exp(-dt_step[:, None, :] * jnp.exp(a_log[layer])[None])
    fresh_state = decay_rate * ssm_state[layer] + (dt_step * widened)[:, None, :] * b_in[:, :, None]
    readout = jnp.sum(fresh_state * c_out[:, :, None], axis=1) + skip_gain[layer][None, :] * widened
    gated_out = (readout * jax.nn.silu(gate_half.astype(jnp.float32))).astype(jnp.bfloat16)
    return (gated_out, fresh_state, window[:, 1:, :])


def attend(scaled, squares, model_dim, asker_lookup_matrix, kv_cache, lengths, page_table):
    requests = scaled.shape[0]
    heads_kv = asker_lookup_matrix.shape[1]
    per_lens_width = kv_cache.shape[4]
    group_size = asker_lookup_matrix.shape[2] // per_lens_width - 2
    inv_sqrt = per_lens_width ** (-0.5)
    qkv_terms = jnp.einsum(
        "bd,dkc->bkc", scaled, asker_lookup_matrix, preferred_element_type=jnp.float32
    )
    qkv_sum, square_sum = seq_sum(qkv_terms, squares, 12)
    inv_rms = lax.rsqrt(square_sum / model_dim + norm_eps)
    qkv_all = lax.optimization_barrier((qkv_sum * inv_rms[:, None, None]).astype(jnp.bfloat16))
    every_question = qkv_all[:, :, : group_size * per_lens_width].reshape(
        requests, heads_kv, group_size, per_lens_width
    )
    newest_pair = qkv_all[:, :, group_size * per_lens_width :].reshape(
        requests, heads_kv, 2, per_lens_width
    )
    pages_dev = kv_cache.shape[0]
    block_len = kv_cache.shape[1]
    slot_ids = lax.axis_index("seq") * pages_dev + jnp.arange(pages_dev, dtype=jnp.int32)
    matches = page_table[:, :, None] == slot_ids[None, None, :]
    belongs = jnp.any(matches, axis=1)
    in_use = jnp.any(belongs, axis=0)
    owner_req = jnp.sum(
        jnp.where(belongs, jnp.arange(requests, dtype=jnp.int32)[:, None], 0), axis=0
    )
    page_index = jnp.sum(
        jnp.where(matches, jnp.arange(page_table.shape[1], dtype=jnp.int32)[None, :, None], 0),
        axis=(0, 1),
    )
    filled = jnp.where(
        in_use, jnp.clip(lengths[owner_req] - page_index * block_len, 0, block_len), 0
    )
    live_count = jnp.sum(in_use.astype(jnp.int32))
    per_step = max(1, 512 // block_len)
    padded = -(-pages_dev // per_step) * per_step
    slot_order = jnp.argsort(
        jnp.where(in_use, 0, pages_dev) + jnp.arange(pages_dev, dtype=jnp.int32)
    )
    slot_order = jnp.concatenate([slot_order, jnp.zeros((padded - pages_dev,), jnp.int32)])
    live_lane = jnp.arange(padded, dtype=jnp.int32) < live_count
    lane_fill = jnp.where(live_lane, filled[slot_order], 0)
    lane_owner = owner_req[slot_order]

    def visit(index_step, carried):
        page_tops, page_sums, page_accs = carried
        first_lane = index_step * per_step
        slots_now = lax.dynamic_slice_in_dim(slot_order, first_lane, per_step)
        fills_now = lax.dynamic_slice_in_dim(lane_fill, first_lane, per_step)
        owners_now = lax.dynamic_slice_in_dim(lane_owner, first_lane, per_step)
        page_rows = kv_cache[slots_now]
        queries = every_question[owners_now]
        scores = (
            jnp.einsum(
                "pkgd,ptkd->pkgt", queries, page_rows[:, :, 0], preferred_element_type=jnp.float32
            )
            * inv_sqrt
        )
        visible = (
            jnp.arange(block_len, dtype=jnp.int32)[None, None, None, :]
            < fills_now[:, None, None, None]
        )
        scores = jnp.where(visible, scores, lowest_score)
        block_top = jnp.max(scores, axis=3)
        weight = jnp.where(visible, jnp.exp(scores - block_top[..., None]), 0.0)
        block_sum = jnp.sum(weight, axis=3)
        values = jnp.einsum(
            "pkgt,ptkd->pkgd",
            weight.astype(jnp.bfloat16),
            page_rows[:, :, 1],
            preferred_element_type=jnp.float32,
        )
        return (
            lax.dynamic_update_slice_in_dim(page_tops, block_top, first_lane, 0),
            lax.dynamic_update_slice_in_dim(page_sums, block_sum, first_lane, 0),
            lax.dynamic_update_slice_in_dim(page_accs, values, first_lane, 0),
        )

    start_state = (
        jnp.full((padded, heads_kv, group_size), lowest_score, jnp.float32),
        jnp.zeros((padded, heads_kv, group_size), jnp.float32),
        jnp.zeros((padded, heads_kv, group_size, per_lens_width), jnp.float32),
    )
    step_count = (live_count + per_step - 1) // per_step
    page_tops, page_sums, page_accs = lax.fori_loop(0, step_count, visit, start_state)
    selects = (lane_owner[None, :] == jnp.arange(requests, dtype=jnp.int32)[:, None]) & live_lane[
        None, :
    ]
    chosen = selects[:, :, None, None]
    local_top = jnp.max(jnp.where(chosen, page_tops[None], lowest_score), axis=1)
    factor = jnp.where(chosen, jnp.exp(page_tops[None] - local_top[:, None]), 0.0)
    local_sum = jnp.sum(factor * page_sums[None], axis=1)
    local_acc = jnp.einsum("bpkg,pkgd->bkgd", factor, page_accs, precision=lax.Precision.HIGHEST)
    packed = jnp.stack([local_top, local_sum]).reshape(2, -1)
    accs_all, packed_all = seq_collect(
        local_acc.astype(wire).reshape(-1, per_lens_width), packed, 13
    )
    seq = accs_all.shape[0]
    tops = packed_all[:, 0].reshape((seq,) + local_top.shape)
    sums = packed_all[:, 1].reshape((seq,) + local_top.shape)
    accs = accs_all.reshape((seq,) + local_acc.shape).astype(jnp.float32)
    grand_top = jnp.max(tops, axis=0)
    rescale = jnp.exp(tops - grand_top[None])
    weight_total = jnp.sum(sums * rescale, axis=0)
    value_total = jnp.sum(accs * rescale[..., None], axis=0)
    fresh_score = (
        jnp.einsum(
            "ujqf,ujf->ujq",
            every_question,
            newest_pair[:, :, 0],
            preferred_element_type=jnp.float32,
        )
        * inv_sqrt
    )
    final_top = jnp.maximum(grand_top, fresh_score)
    carry_old = jnp.exp(grand_top - final_top)
    fresh_weight = jnp.exp(fresh_score - final_top)
    denominator = weight_total * carry_old + fresh_weight
    numerator = value_total * carry_old[..., None] + fresh_weight[..., None] * newest_pair[:, :, 1][
        :, :, None, :
    ].astype(jnp.float32)
    attended = (numerator / denominator[..., None]).astype(jnp.bfloat16)
    return (attended.reshape(requests, heads_kv, group_size * per_lens_width), newest_pair)


def shards(
    hidden,
    norm_gain,
    in_weight,
    conv_weight,
    conv_bias,
    conv_state,
    xproj_weight,
    dt_weight,
    dt_bias,
    a_log,
    skip_gain,
    ssm_state,
    out_weight,
    asker_lookup_matrix,
    o_weight,
    kv_cache,
    lengths,
    page_table,
):
    layer_params = (
        in_weight,
        conv_weight,
        conv_bias,
        conv_state,
        xproj_weight,
        dt_weight,
        dt_bias,
        a_log,
        skip_gain,
        ssm_state,
    )
    model_dim = hidden.shape[1]
    share_cols = model_dim // lax.axis_size(("seq", "chan"))
    block_cols = model_dim // lax.axis_size("seq")
    seq_index = lax.axis_index("seq")
    share_index = seq_index * lax.axis_size("chan") + lax.axis_index("chan")
    normed = normalize(hidden, norm_gain[0])
    gated_first, state_first, conv_first = mamba_mix(normed, 0, layer_params)
    first_terms = jnp.dot(gated_first, out_weight[0], preferred_element_type=jnp.float32)
    hidden_share = lax.dynamic_slice_in_dim(hidden, share_index * share_cols, share_cols, 1)
    stream_one, block = share_sum(first_terms, hidden_share, True, 14)
    widened = block.transpose(1, 0, 2).reshape(hidden.shape[0], block_cols).astype(jnp.float32)
    gain_block = lax.dynamic_slice_in_dim(norm_gain[1], seq_index * block_cols, block_cols, 0)
    scaled = (widened * gain_block[None, :]).astype(jnp.bfloat16)
    squares = jnp.sum(widened * widened, axis=1)
    attended, newest_pair = attend(
        scaled, squares, model_dim, asker_lookup_matrix, kv_cache, lengths, page_table
    )
    attn_terms = jnp.einsum("khc,bkh->bc", o_weight, attended, preferred_element_type=jnp.float32)
    stream_two, every = chan_sum(attn_terms, stream_one, 15)
    normed_two = normalize(every, norm_gain[2])
    gated_two, state_two, conv_two = mamba_mix(normed_two, 1, layer_params)
    last_terms = jnp.dot(gated_two, out_weight[1], preferred_element_type=jnp.float32)
    (hidden_out,) = share_sum(last_terms, stream_two, False, 16)
    return (
        hidden_out,
        jnp.stack([state_first, state_two]),
        jnp.stack([conv_first, conv_two]),
        newest_pair,
    )


def solution(mesh):
    in_specs = (
        P(),
        P(),
        P(None, None, None, ("seq", "chan")),
        P(None, None, ("seq", "chan")),
        P(None, ("seq", "chan")),
        P(None, None, None, ("seq", "chan")),
        P(None, ("seq", "chan"), None),
        P(None, None, ("seq", "chan")),
        P(None, ("seq", "chan")),
        P(None, None, ("seq", "chan")),
        P(None, ("seq", "chan")),
        P(None, None, None, ("seq", "chan")),
        P(None, ("seq", "chan"), None),
        P("seq", "chan", None),
        P("chan", None, "seq"),
        P("seq", None, None, "chan", None),
        P(),
        P(),
    )
    out_specs = (
        P(None, ("seq", "chan")),
        P(None, None, None, ("seq", "chan")),
        P(None, None, None, ("seq", "chan")),
        P(None, "chan", None, None),
    )
    return jax.shard_map(shards, mesh=mesh, in_specs=in_specs, out_specs=out_specs, check_vma=False)
```
